768 devices in a mesh: ta: 192 (over x, y, z_lo, core), gz: 4 (over z_hi).
Axes of the slice: x: 4, y: 8, z: 12 (z_hi: 4, z_lo: 3; z = z_hi * 3 + z_lo), core: 2. Of those that a mesh axis runs over, the one named last changes fastest.
Arguments:
- spinor: float32 [2, 4, 3, 384, 8, 768], P(None, None, None, 'ta', 'gz'), may hold values from -3 to 3
- links: float32 [4, 2, 3, 3, 384, 8, 768], P(None, None, None, None, 'ta', 'gz'), may hold values from -3.5 to 3.5
- clover: float32 [2, 2, 6, 6, 384, 8, 768], P(None, None, None, None, 'ta', 'gz'), may hold values from -1.2 to 1.2
Outputs:
- applied: float32 [2, 4, 3, 384, 8, 768], P(None, None, None, 'ta', 'gz')
- force: float32 [4, 2, 3, 3, 384, 8, 768], P(None, None, None, None, 'ta', 'gz')
The draws below stay inside these ranges and needn't reach their ends.
All inputs are finite; a program needn't handle non-finite values.
Results may differ from the reference program's by a relative error of at most 0.0001.
Values sent between devices are 32-bit elements; how exact they have to be, the bound alone decides.
No kernel may reach another device: no remote copies, remote signals or barrier semaphores. Data moves between devices by JAX's collectives and lax.ppermute only.
A program may use at most 64 MiB of HBM per device.

```python
import jax
import jax.numpy as jnp

NY = 12
NX = 64
PLANE = 768
NT = 384
NZ = 8


def shard_levels(stream_key, extent, pieces, least, largest):
    def one(dim, shards_of):
        heights = jax.random.uniform(jax.random.fold_in(jax.random.fold_in(stream_key, 6), dim), (shards_of,), jnp.float32, least / len(pieces), largest / len(pieces))
        return jnp.repeat(jnp.exp(heights), extent[dim] // shards_of).reshape((-1,) + (1,) * (len(extent) - dim - 1))

    gain = one(*pieces[0])
    for cut in pieces[1:]:
        gain = gain * one(*cut)
    return gain


def centred(key, extent, spread, limit, shards=(), kind=jnp.bfloat16):
    array = jax.random.normal(key, extent, jnp.float32) * spread
    if len(shards) > 0:
        array = shard_levels(key, extent, shards, -0.22, 0.18) * array
    return jnp.clip(array, min=-limit, max=limit).astype(kind)


def setup_inputs(seed: int = 0) -> dict:
    key_of = jax.random.split(jax.random.key(seed), 4)
    spinor = centred(key_of[0], (2, 4, 3, NT, NZ, PLANE), 0.5, 3.0, ((3, 192), (4, 4)), jnp.float32)
    links = centred(key_of[1], (4, 2, 3, 3, NT, NZ, PLANE), 3 ** -0.5, 3.5, ((4, 192), (5, 4)), jnp.float32)
    clover = centred(key_of[2], (2, 2, 6, 6, NT, NZ, PLANE), 0.2, 1.2, ((4, 192), (5, 4)), jnp.float32)
    return {"spinor": spinor, "links": links, "clover": clover}


bare_mass = -0.25

gamma_table = (
    ((3, 0.0, -1.0), (2, 0.0, -1.0), (1, 0.0, 1.0), (0, 0.0, 1.0)),
    ((3, -1.0, 0.0), (2, 1.0, 0.0), (1, 1.0, 0.0), (0, -1.0, 0.0)),
    ((2, 0.0, -1.0), (3, 0.0, 1.0), (0, 0.0, 1.0), (1, 0.0, -1.0)),
    ((2, 1.0, 0.0), (3, 1.0, 0.0), (0, 1.0, 0.0), (1, 1.0, 0.0)),
)


def apply_gamma(hop_dir, field):
    parts_re = []
    parts_im = []
    for spin_row in range(4):
        source, phase_re, phase_im = gamma_table[hop_dir][spin_row]
        source_re = field[0, source]
        source_im = field[1, source]
        if phase_im == 0.0:
            parts_re.append(phase_re * source_re)
            parts_im.append(phase_re * source_im)
        else:
            parts_re.append(-phase_im * source_im)
            parts_im.append(phase_im * source_re)
    return jnp.stack([jnp.stack(parts_re), jnp.stack(parts_im)])


def project(hop_dir, field, sign):
    return field + sign * apply_gamma(hop_dir, field)


def color_apply(link, field, dagger):
    link_re = link[0]
    link_im = link[1]
    if dagger:
        link_re = jnp.swapaxes(link_re, 0, 1)
        link_im = -jnp.swapaxes(link_im, 0, 1)
    matrix_re = link_re[None]
    matrix_im = link_im[None]
    field_re = field[0][:, None]
    field_im = field[1][:, None]
    out_re = jnp.sum(matrix_re * field_re - matrix_im * field_im, axis=2)
    out_im = jnp.sum(matrix_re * field_im + matrix_im * field_re, axis=2)
    return jnp.stack([out_re, out_im])


def clover_apply(clover, field):
    halves = field.reshape((2, 2, 6) + field.shape[3:])
    field_re = halves[0][:, None]
    field_im = halves[1][:, None]
    out_re = jnp.sum(clover[0] * field_re - clover[1] * field_im, axis=2)
    out_im = jnp.sum(clover[0] * field_im + clover[1] * field_re, axis=2)
    return jnp.stack([out_re, out_im]).reshape(field.shape)


def spin_outer(left, right):
    left_re = left[0][:, :, None]
    left_im = left[1][:, :, None]
    right_re = right[0][:, None]
    right_im = right[1][:, None]
    out_re = jnp.sum(left_re * right_re + left_im * right_im, axis=0)
    out_im = jnp.sum(left_im * right_re - left_re * right_im, axis=0)
    return jnp.stack([out_re, out_im])


def color_product(first, second):
    first_re = first[0][:, :, None]
    first_im = first[1][:, :, None]
    second_re = second[0][None]
    second_im = second[1][None]
    out_re = jnp.sum(first_re * second_re - first_im * second_im, axis=1)
    out_im = jnp.sum(first_re * second_im + first_im * second_re, axis=1)
    return jnp.stack([out_re, out_im])


def traceless(matrix):
    mat_re = matrix[0]
    mat_im = matrix[1]
    anti_re = 0.5 * (mat_re - jnp.swapaxes(mat_re, 0, 1))
    anti_im = 0.5 * (mat_im + jnp.swapaxes(mat_im, 0, 1))
    trace_third = (mat_im[0, 0] + mat_im[1, 1] + mat_im[2, 2]) / 3.0
    identity = jnp.eye(3, dtype=jnp.float32).reshape((3, 3) + (1,) * (mat_re.ndim - 2))
    return jnp.stack([anti_re, anti_im - identity * trace_third])


def along_plane(field, hop_dir, step):
    shape = field.shape
    grid = field.reshape(shape[:-1] + (NY, NX))
    if hop_dir == 0:
        grid = jnp.roll(grid, -step, axis=-1)
    else:
        grid = jnp.roll(grid, -step, axis=-2)
    return grid.reshape(shape)


def neighbor(field, hop_dir, step, fermion):
    if hop_dir < 2:
        return along_plane(field, hop_dir, step)
    if hop_dir == 2:
        return jnp.roll(field, -step, axis=4)
    moved = jnp.roll(field, -step, axis=3)
    if fermion:
        boundary = field.shape[3] - 1 if step == 1 else 0
        moved = moved.at[:, :, :, boundary].multiply(-1.0)
    return moved


def reference(spinor, links, clover):
    hopping = jnp.zeros_like(spinor)
    forward_half = []
    for hop_dir in range(4):
        ahead_proj = project(hop_dir, neighbor(spinor, hop_dir, 1, True), -1.0)
        forward_half.append(ahead_proj)
        behind = neighbor(spinor, hop_dir, -1, True)
        back_link = neighbor(links[hop_dir], hop_dir, -1, False)
        hopping = hopping + color_apply(links[hop_dir], ahead_proj, False) + color_apply(back_link, project(hop_dir, behind, 1.0), True)
    applied = (4.0 + bare_mass) * spinor + clover_apply(clover, spinor) - 0.5 * hopping
    forces = []
    for hop_dir in range(4):
        ahead_applied = neighbor(applied, hop_dir, 1, True)
        summed = spin_outer(forward_half[hop_dir], applied) + spin_outer(project(hop_dir, ahead_applied, 1.0), spinor)
        forces.append(traceless(color_product(links[hop_dir], summed)))
    return applied, jnp.stack(forces)
```

```python
import jax
import jax.numpy as jnp
from jax import lax
from jax.experimental import pallas as pl
from jax.experimental.pallas import tpu as pltpu
from jax.sharding import PartitionSpec as P


F32 = jnp.float32
LANES = 128
DIAG = 3.75
PAIRED = ('ta', 'gz')
gamma_table = (
    ((3, 0, -1), (2, 0, -1), (1, 0, 1), (0, 0, 1)),
    ((3, -1, 0), (2, 1, 0), (1, 1, 0), (0, -1, 0)),
    ((2, 0, -1), (3, 0, 1), (0, 0, 1), (1, 0, -1)),
    ((2, 1, 0), (3, 1, 0), (0, 1, 0), (1, 1, 0)),
)


def add(x, y, sign):
    return x + y if sign > 0 else x - y


def half(psi, mu, sign):
    out = []
    for s in range(2):
        src, pr, pi = gamma_table[mu][s]
        row = []
        for a in range(3):
            re, im = psi[s][a]
            sre, sim = psi[src][a]
            if pi == 0:
                row.append((add(re, sre, sign * pr), add(im, sim, sign * pr)))
            else:
                row.append((add(re, sim, -sign * pi), add(im, sre, sign * pi)))
        out.append(row)
    return out


def phase(mu, r, h):
    src, pr, pi = gamma_table[mu][r]
    if pi == 0:
        return [((pr, re), (pr, im)) for re, im in h[src]]
    return [((-pi, im), (pi, re)) for re, im in h[src]]


def cmul(u, h):
    out = []
    for s in range(2):
        row = []
        for a in range(3):
            re = im = None
            for b in range(3):
                ur, ui = u[a][b]
                hr, hi = h[s][b]
                r = ur * hr - ui * hi
                i = ur * hi + ui * hr
                re = r if re is None else re + r
                im = i if im is None else im + i
            row.append((re, im))
        out.append(row)
    return out


def cmul_dag(u, h):
    out = []
    for s in range(2):
        row = []
        for a in range(3):
            re = im = None
            for b in range(3):
                ur, ui = u[b][a]
                hr, hi = h[s][b]
                r = ur * hr + ui * hi
                i = ur * hi - ui * hr
                re = r if re is None else re + r
                im = i if im is None else im + i
            row.append((re, im))
        out.append(row)
    return out


def hmap(f, h):
    return [[(f(re), f(im)) for re, im in row] for row in h]


def hmap2(f, g, h):
    return [[(f(x[0], y[0]), f(x[1], y[1])) for x, y in zip(p, q)] for p, q in zip(g, h)]


def accumulate(acc, mu, h, sign):
    for s in range(2):
        for a in range(3):
            acc[s][a] = (acc[s][a][0] + h[s][a][0], acc[s][a][1] + h[s][a][1])
    signed = h if isinstance(sign, int) else hmap(lambda v: v * sign, h)
    flip = sign if isinstance(sign, int) else 1
    for r in range(2, 4):
        for a, ((gr, vr), (gi, vi)) in enumerate(phase(mu, r, signed)):
            acc[r][a] = (add(acc[r][a][0], vr, flip * gr), add(acc[r][a][1], vi, flip * gi))


def rows_of(k):
    return slice(8 * k, 8 * k + 8)


def get_spinor(ref, index):
    return [[(ref[3 * s + a, index, :], ref[12 + 3 * s + a, index, :]) for a in range(3)] for s in range(4)]


def get_link(ref, d, index):
    return [[(ref[18 * d + 3 * a + b, index, :], ref[18 * d + 9 + 3 * a + b, index, :]) for b in range(3)] for a in range(3)]


def get_half(ref, index):
    return [[(ref[3 * s + a, index, :], ref[6 + 3 * s + a, index, :]) for a in range(3)] for s in range(2)]


def put_half(ref, index, h):
    for s in range(2):
        for a in range(3):
            ref[3 * s + a, index, :] = h[s][a][0]
            ref[6 + 3 * s + a, index, :] = h[s][a][1]


def put_spinor(ref, index, psi):
    for s in range(4):
        for a in range(3):
            ref[3 * s + a, index, :] = psi[s][a][0]
            ref[12 + 3 * s + a, index, :] = psi[s][a][1]


def iotas():
    lane = lax.broadcasted_iota(jnp.int32, (8, LANES), 1)
    row = lax.broadcasted_iota(jnp.int32, (8, LANES), 0)
    return lane, row


def shift_x(v, step):
    lane = lax.broadcasted_iota(jnp.int32, (8, LANES), 1) % 64
    if step > 0:
        return jnp.where(lane == 63, pltpu.roll(v, 63, 1), pltpu.roll(v, LANES - 1, 1))
    return jnp.where(lane == 0, pltpu.roll(v, 65, 1), pltpu.roll(v, 1, 1))


def shift_y(here, other, step):
    lane, row = iotas()
    low = row < 4
    mixed = jnp.where(low, other, here) if step > 0 else jnp.where(low, here, other)
    keep = lane >= 64 if step > 0 else lane < 64
    return pltpu.roll(jnp.where(keep, here, pltpu.roll(mixed, 4, 0)), 64, 1)


def shift_rows(v, count, step):
    return pltpu.roll(v, 8 - count if step > 0 else count, 0)


def is_even(axis):
    return lax.axis_index(axis) % 2 == 0


def outgoing(axis, up, dn):
    if axis not in PAIRED:
        return up, dn
    even = is_even(axis)
    return jnp.where(even, up, dn), jnp.where(even, dn, up)


def sent_up(axis, first, second, index):
    if axis not in PAIRED:
        return first[index]
    return jnp.where(is_even(axis), first[index], second[index])


def from_below(axis, first, second, index):
    if axis not in PAIRED:
        return first[index]
    return jnp.where(is_even(axis), second[index], first[index])


def from_above(axis, first, second, index):
    if axis not in PAIRED:
        return second[index]
    return jnp.where(is_even(axis), first[index], second[index])


def plane_copies(src, dst, sems, out=False):
    copies = []
    tiles = dst.shape[-3] // 2
    lead = (slice(None),) * (len(dst.shape) - 3)
    for t in range(2):
        for j in range(tiles):
            wide = src.at[lead + (t, slice(None), pl.ds(LANES * j, LANES))]
            packed = dst.at[lead + (2 * j + t,)]
            pair = (packed, wide) if out else (wide, packed)
            copies.append(pltpu.make_async_copy(*pair, sems.at[2 * j + t]))
    return copies


def flat(ref):
    shape = ref.shape
    lead = 1
    for n in shape[:-3]:
        lead *= n
    return ref.reshape(lead, 2 * shape[-3], LANES)


def put_face(ref, part, h):
    for s in range(2):
        for a in range(3):
            ref[pl.ds(12 * (3 * s + a) + 6 * part, 6), :] = h[s][a][0]
            ref[pl.ds(12 * (6 + 3 * s + a) + 6 * part, 6), :] = h[s][a][1]


def face_rows(t, z):
    return pl.ds(2 * t + z, 6, stride=4)


def halo_row(c, part):
    return (pl.ds(12 * c + 6 * part, 6), slice(None))


def faces_kernel(spinor, links, s_out, l_out, t_a, t_b, z_a, z_b, sem_s, sem_l):
    copies = plane_copies(spinor, s_out, sem_s) + plane_copies(links.at[pl.ds(2, 2)], l_out, sem_l)
    for c in copies:
        c.start()
    place = lax.axis_index("ta")
    up_sign = jnp.where(place == lax.axis_size("ta") - 1, -1.0, 1.0).astype(F32)
    dn_sign = jnp.where(place == 0, -1.0, 1.0).astype(F32)
    for c in copies:
        c.wait()
    s_ref, l_ref = flat(s_out), flat(l_out)
    for part in range(2):
        for axis, mu, d, first, second, low, high in (
            ("gz", 2, 0, z_a, z_b, face_rows(part, 0), face_rows(part, 1)),
            ("ta", 3, 1, t_a, t_b, face_rows(0, part), face_rows(1, part)),
        ):
            dn = half(get_spinor(s_ref, low), mu, -1)
            up = cmul_dag(get_link(l_ref, d, high), half(get_spinor(s_ref, high), mu, 1))
            if axis == "ta":
                dn = hmap(lambda v: v * dn_sign, dn)
                up = hmap(lambda v: v * up_sign, up)
            put_face(first, part, hmap2(lambda x, y: outgoing(axis, x, y)[0], up, dn))
            put_face(second, part, hmap2(lambda x, y: outgoing(axis, x, y)[1], up, dn))


def local_kernel(s_in, l_in, links, clover, p_out, l_out, c_ref, chi, sem_l, sem_c):
    copies_l = plane_copies(links.at[pl.ds(0, 2)], l_out, sem_l)
    copies_c = plane_copies(clover, c_ref, sem_c)
    for c in copies_l + copies_c:
        c.start()
    s_ref, l23, l01, cl = flat(s_in), flat(l_in), flat(l_out), flat(c_ref)
    _, row = iotas()
    low_z = row % 2 == 0
    low_t = (row // 2) % 2 == 0
    sign_z = jnp.where(low_z, -1.0, 1.0)
    sign_t = jnp.where(low_t, -1.0, 1.0)
    zero = jnp.zeros((8, LANES), F32)
    for k in range(3):
        psi = get_spinor(s_ref, rows_of(k))
        acc = [[(zero, zero) for _ in range(3)] for _ in range(4)]
        for mu, d, n, low, sign in ((2, 0, 1, low_z, sign_z), (3, 1, 2, low_t, sign_t)):
            u = get_link(l23, d, rows_of(k))
            ahead = cmul(u, hmap(lambda v: shift_rows(v, n, 1), half(psi, mu, -1)))
            behind = hmap(lambda v: shift_rows(v, n, -1), cmul_dag(u, half(psi, mu, 1)))
            accumulate(acc, mu, hmap2(lambda x, y: jnp.where(low, x, y), ahead, behind), sign)
        put_spinor(p_out, rows_of(k), acc)
    for c in copies_l:
        c.wait()
    for k in range(3):
        put_half(chi, rows_of(k), cmul_dag(get_link(l01, 1, rows_of(k)), half(get_spinor(s_ref, rows_of(k)), 1, 1)))
    for k in range(3):
        psi = get_spinor(s_ref, rows_of(k))
        acc = get_spinor(p_out, rows_of(k))
        u = get_link(l01, 0, rows_of(k))
        accumulate(acc, 0, cmul(u, hmap(lambda v: shift_x(v, 1), half(psi, 0, -1))), -1)
        accumulate(acc, 0, hmap(lambda v: shift_x(v, -1), cmul_dag(u, half(psi, 0, 1))), 1)
        u = get_link(l01, 1, rows_of(k))
        nxt = half(get_spinor(s_ref, rows_of((k + 1) % 3)), 1, -1)
        ahead = hmap2(lambda x, y: shift_y(x, y, 1), half(psi, 1, -1), nxt)
        accumulate(acc, 1, cmul(u, ahead), -1)
        behind = hmap2(lambda x, y: shift_y(x, y, -1), get_half(chi, rows_of(k)), get_half(chi, rows_of((k + 2) % 3)))
        accumulate(acc, 1, behind, 1)
        put_spinor(p_out, rows_of(k), acc)
    for c in copies_c:
        c.wait()
    for k in range(3):
        for chirality in range(2):
            field = [[(s_ref[6 * chirality + i, rows_of(k), :], s_ref[12 + 6 * chirality + i, rows_of(k), :])] for i in range(6)]
            for i in range(6):
                re = DIAG * field[i][0][0] - 0.5 * p_out[6 * chirality + i, rows_of(k), :]
                im = DIAG * field[i][0][1] - 0.5 * p_out[12 + 6 * chirality + i, rows_of(k), :]
                for j in range(6):
                    cr = cl[36 * chirality + 6 * i + j, rows_of(k), :]
                    ci = cl[72 + 36 * chirality + 6 * i + j, rows_of(k), :]
                    fr, fi = field[j][0]
                    re = re + (cr * fr - ci * fi)
                    im = im + (cr * fi + ci * fr)
                p_out[6 * chirality + i, rows_of(k), :] = re
                p_out[12 + 6 * chirality + i, rows_of(k), :] = im


def low_rows(mu):
    row = lax.broadcasted_iota(jnp.int32, (8, LANES), 0)
    return (row if mu == 2 else row // 2) % 2 == 0


def spread(dst, mu, level, value):
    for c in range(12):
        for part in range(2):
            first = 2 * part + level if mu == 2 else 2 * level + part
            dst[c, pl.ds(first, 6, stride=4), :] = value(c, part)


def add_halo(acc, mu, u, h):
    low = low_rows(mu)
    term = hmap2(lambda x, y: -0.5 * jnp.where(low, x, y), h, cmul(u, h))
    accumulate(acc, mu, term, jnp.where(low, 1.0, -1.0))


def halo_kernel(mu, p_in, l_in, first, second, a_out, face, halo):
    axis = "gz" if mu == 2 else "ta"
    l23 = flat(l_in)
    a_ref = flat(a_out) if len(a_out.shape) > 3 else a_out
    spread(halo, mu, 0, lambda c, part: from_below(axis, first, second, halo_row(c, part)))
    spread(halo, mu, 1, lambda c, part: from_above(axis, first, second, halo_row(c, part)))
    for k in range(3):
        acc = get_spinor(p_in, rows_of(k))
        add_halo(acc, mu, get_link(l23, mu - 2, rows_of(k)), get_half(halo, rows_of(k)))
        put_spinor(a_ref, rows_of(k), acc)
    dn_sign = jnp.where(lax.axis_index("ta") == 0, -1.0, 1.0).astype(F32)
    for part in range(2):
        if mu == 3:
            put_face(face, part, half(get_spinor(a_ref, face_rows(part, 0)), 2, 1))
        else:
            out = half(get_spinor(a_ref, face_rows(0, part)), 3, 1)
            put_face(face, part, hmap(lambda v: v * dn_sign, out))


def mid_kernel(*refs):
    halo_kernel(3, *refs)


def finish_kernel(*refs):
    halo_kernel(2, *refs)


def outer(left, right, total=None):
    out = []
    for a in range(3):
        row = []
        for b in range(3):
            re, im = (None, None) if total is None else total[a][b]
            for s in range(2):
                lr, li = left[s][a]
                rr, ri = right[s][b]
                r = lr * rr + li * ri
                i = li * rr - lr * ri
                re = r if re is None else re + r
                im = i if im is None else im + i
            row.append((re, im))
        out.append(row)
    return out


def put_force(ref, d, index, u, m):
    w = []
    for a in range(3):
        row = []
        for b in range(3):
            re = im = None
            for c in range(3):
                ur, ui = u[a][c]
                mr, mi = m[c][b]
                i = ur * mi + ui * mr
                im = i if im is None else im + i
                if a != b:
                    r = ur * mr - ui * mi
                    re = r if re is None else re + r
            row.append((re, im))
        w.append(row)
    third = (w[0][0][1] + w[1][1][1] + w[2][2][1]) * (1.0 / 3.0)
    for a in range(3):
        ref[18 * d + 4 * a, index, :] = jnp.zeros((8, LANES), F32)
        ref[18 * d + 9 + 4 * a, index, :] = w[a][a][1] - third
        for b in range(a + 1, 3):
            re = 0.5 * (w[a][b][0] - w[b][a][0])
            im = 0.5 * (w[a][b][1] + w[b][a][1])
            ref[18 * d + 3 * a + b, index, :] = re
            ref[18 * d + 3 * b + a, index, :] = -re
            ref[18 * d + 9 + 3 * a + b, index, :] = im
            ref[18 * d + 9 + 3 * b + a, index, :] = im


def get_matrix(ref, d, index):
    return get_link(ref, d, index)


def put_matrix(ref, d, index, m):
    for a in range(3):
        for b in range(3):
            ref[18 * d + 3 * a + b, index, :] = m[a][b][0]
            ref[18 * d + 9 + 3 * a + b, index, :] = m[a][b][1]


def plane_kernel(s_in, a_in, l_in, t_a, t_b, z_a, z_b, applied, force, m_out, f_ref, halo, sem_a, sem_f):
    copies = plane_copies(applied, a_in, sem_a, out=True)
    for c in copies:
        c.start()
    s_ref, a_ref, l01, f = flat(s_in), flat(a_in), flat(l_in), flat(f_ref)
    for k in range(3):
        psi = get_spinor(s_ref, rows_of(k))
        app = get_spinor(a_ref, rows_of(k))
        m = outer(hmap(lambda v: shift_x(v, 1), half(psi, 0, -1)), half(app, 0, -1))
        m = outer(hmap(lambda v: shift_x(v, 1), half(app, 0, 1)), half(psi, 0, 1), m)
        put_force(f, 0, rows_of(k), get_link(l01, 0, rows_of(k)), m)
        psi_n = half(get_spinor(s_ref, rows_of((k + 1) % 3)), 1, -1)
        app_n = half(get_spinor(a_ref, rows_of((k + 1) % 3)), 1, 1)
        m = outer(hmap2(lambda x, y: shift_y(x, y, 1), half(psi, 1, -1), psi_n), half(app, 1, -1))
        m = outer(hmap2(lambda x, y: shift_y(x, y, 1), half(app, 1, 1), app_n), half(psi, 1, 1), m)
        put_force(f, 1, rows_of(k), get_link(l01, 1, rows_of(k)), m)
    out = plane_copies(force.at[pl.ds(0, 2)], f_ref, sem_f, out=True)
    for c in out:
        c.start()
    for mu, axis, first, second in ((2, "gz", z_a, z_b), (3, "ta", t_a, t_b)):
        low = low_rows(mu)
        spread(halo, mu, 1, lambda c, part: from_above(axis, first, second, halo_row(c, part)))
        for k in range(3):
            psi = get_spinor(s_ref, rows_of(k))
            app = get_spinor(a_ref, rows_of(k))
            near = hmap(lambda v: shift_rows(v, mu - 1, 1), half(psi, mu, -1))
            ahead = hmap2(lambda x, y: jnp.where(low, x, y), near, get_half(halo, rows_of(k)))
            m = outer(ahead, half(app, mu, -1))
            ahead = hmap(lambda v: jnp.where(low, shift_rows(v, mu - 1, 1), 0.0), half(app, mu, 1))
            m = outer(ahead, half(psi, mu, 1), m)
            put_matrix(m_out, mu - 2, rows_of(k), m)
    for c in copies + out:
        c.wait()


def edge_kernel(s_in, l_in, m_in, a_t, a_z, z_a, z_b, force_in, force, f_ref, halo, sem_f):
    s_ref, l23, f = flat(s_in), flat(l_in), flat(f_ref)
    out = []
    for d, mu in ((1, 3), (0, 2)):
        for c in range(12):
            for k in range(3):
                halo[c, rows_of(k), :] = jnp.zeros((8, LANES), F32)
        if mu == 3:
            spread(halo, mu, 1, lambda c, part: a_t[halo_row(c, part)])
        else:
            spread(halo, mu, 1, lambda c, part: a_z[halo_row(c, part)] - sent_up("gz", z_a, z_b, halo_row(c, part)))
        for k in range(3):
            psi = half(get_spinor(s_ref, rows_of(k)), mu, 1)
            m = outer(get_half(halo, rows_of(k)), psi, get_matrix(m_in, d, rows_of(k)))
            put_force(f, d, rows_of(k), get_link(l23, d, rows_of(k)), m)
        copies = plane_copies(force.at[pl.ds(mu, 1)], f_ref.at[pl.ds(d, 1)], sem_f.at[d], out=True)
        for c in copies:
            c.start()
        out += copies
    for c in out:
        c.wait()


HBM = pl.BlockSpec(memory_space=pltpu.HBM)
VMEM = pl.BlockSpec(memory_space=pltpu.VMEM)
LIMIT = 12 * 1024 * 1024


def call(kernel, ins, outs, scratch, args, aliases=None):
    return pl.pallas_call(
        kernel,
        out_shape=tuple(jax.ShapeDtypeStruct(shape, F32) for shape, _ in outs),
        in_specs=list(ins),
        out_specs=tuple(spec for _, spec in outs),
        scratch_shapes=list(scratch),
        compiler_params=pltpu.CompilerParams(vmem_limit_bytes=LIMIT),
        input_output_aliases=aliases or {},
    )(*args)


def moved(value, axis, step):
    count = lax.axis_size(axis)
    return lax.ppermute(value, axis, [(i, (i + step) % count) for i in range(count)])


def swapped(value, axis, start):
    count = lax.axis_size(axis)
    pairs = [(i % count, (i + 1) % count) for i in range(start, count + start, 2)]
    return lax.ppermute(value, axis, pairs + [(b, a) for a, b in pairs])


def exchanged(axis, first, second):
    if axis in PAIRED:
        return swapped(first, axis, 0), swapped(second, axis, 1)
    return moved(first, axis, 1), moved(second, axis, -1)


def steps(spinor, links, clover):
    tiles = spinor.shape[-1] // LANES
    packed = (2 * tiles, 2, LANES)
    s_shape = (2, 4, 3) + packed
    l_shape = (2, 2, 3, 3) + packed
    c_shape = (2, 2, 6, 6) + packed
    rows = (4 * tiles, LANES)
    face = ((24 * tiles, LANES), VMEM)
    halo = pltpu.VMEM((12,) + rows, F32)
    dma = pltpu.SemaphoreType.DMA((2 * tiles,))
    spinor, links, clover = (pltpu.with_memory_space_constraint(x, pltpu.HBM) for x in (spinor, links, clover))
    s, l23, t_a, t_b, z_a, z_b = call(
        faces_kernel, (HBM, HBM), ((s_shape, VMEM), (l_shape, VMEM), face, face, face, face),
        (dma, dma), (spinor, links),
    )
    z_sent = (z_a, z_b)
    z_a, z_b = exchanged("gz", z_a, z_b)
    t_a, t_b = exchanged("ta", t_a, t_b)
    p, l01 = call(
        local_kernel, (VMEM, VMEM, HBM, HBM), (((24,) + rows, VMEM), (l_shape, VMEM)),
        (pltpu.VMEM(c_shape, F32), halo, dma, dma), (s, l23, links, clover),
    )
    p, a_z = call(mid_kernel, (VMEM,) * 4, (((24,) + rows, VMEM), face), (halo,), (p, l23, t_a, t_b))
    a_z = moved(a_z, "gz", -1)
    a, a_t = call(finish_kernel, (VMEM,) * 4, ((s_shape, VMEM), face), (halo,), (p, l23, z_a, z_b))
    a_t = moved(a_t, "ta", -1)
    applied, force, m = call(
        plane_kernel, (VMEM,) * 7, ((spinor.shape, HBM), (links.shape, HBM), ((36,) + rows, VMEM)),
        (pltpu.VMEM(l_shape, F32), halo, dma, dma), (s, a, l01, t_a, t_b, z_a, z_b),
    )
    (force,) = call(
        edge_kernel, (VMEM,) * 7 + (HBM,), ((links.shape, HBM),),
        (pltpu.VMEM(l_shape, F32), halo, pltpu.SemaphoreType.DMA((2, 2 * tiles))),
        (s, l23, m, a_t, a_z) + z_sent + (force,), {7: 0},
    )
    return applied, force


def solution(mesh):
    spin = P(None, None, None, "ta", "gz", None)
    link = P(None, None, None, None, "ta", "gz", None)
    return jax.shard_map(steps, mesh=mesh, in_specs=(spin, link, link), out_specs=(spin, link), check_vma=False)
```

```python
import jax
import jax.numpy as jnp
from jax import lax
from jax.experimental import pallas as pl
from jax.experimental.pallas import tpu as pltpu
from jax.sharding import PartitionSpec as P


F32 = jnp.float32
LANES = 128
DIAG = 3.75
gamma_table = (
    ((3, 0, -1), (2, 0, -1), (1, 0, 1), (0, 0, 1)),
    ((3, -1, 0), (2, 1, 0), (1, 1, 0), (0, -1, 0)),
    ((2, 0, -1), (3, 0, 1), (0, 0, 1), (1, 0, -1)),
    ((2, 1, 0), (3, 1, 0), (0, 1, 0), (1, 1, 0)),
)


def add(x, y, sign):
    return x + y if sign > 0 else x - y


def half(psi, mu, sign):
    out = []
    for s in range(2):
        src, pr, pi = gamma_table[mu][s]
        row = []
        for a in range(3):
            re, im = psi[s][a]
            sre, sim = psi[src][a]
            if pi == 0:
                row.append((add(re, sre, sign * pr), add(im, sim, sign * pr)))
            else:
                row.append((add(re, sim, -sign * pi), add(im, sre, sign * pi)))
        out.append(row)
    return out


def phase(mu, r, h):
    src, pr, pi = gamma_table[mu][r]
    if pi == 0:
        return [((pr, re), (pr, im)) for re, im in h[src]]
    return [((-pi, im), (pi, re)) for re, im in h[src]]


def cmul(u, h):
    out = []
    for s in range(2):
        row = []
        for a in range(3):
            re = im = None
            for b in range(3):
                ur, ui = u[a][b]
                hr, hi = h[s][b]
                r = ur * hr - ui * hi
                i = ur * hi + ui * hr
                re = r if re is None else re + r
                im = i if im is None else im + i
            row.append((re, im))
        out.append(row)
    return out


def cmul_dag(u, h):
    out = []
    for s in range(2):
        row = []
        for a in range(3):
            re = im = None
            for b in range(3):
                ur, ui = u[b][a]
                hr, hi = h[s][b]
                r = ur * hr + ui * hi
                i = ur * hi - ui * hr
                re = r if re is None else re + r
                im = i if im is None else im + i
            row.append((re, im))
        out.append(row)
    return out


def hmap(f, h):
    return [[(f(re), f(im)) for re, im in row] for row in h]


def hmap2(f, g, h):
    return [[(f(x[0], y[0]), f(x[1], y[1])) for x, y in zip(p, q)] for p, q in zip(g, h)]


def accumulate(acc, mu, h, sign):
    for s in range(2):
        for a in range(3):
            acc[s][a] = (acc[s][a][0] + h[s][a][0], acc[s][a][1] + h[s][a][1])
    signed = h if isinstance(sign, int) else hmap(lambda v: v * sign, h)
    flip = sign if isinstance(sign, int) else 1
    for r in range(2, 4):
        for a, ((gr, vr), (gi, vi)) in enumerate(phase(mu, r, signed)):
            acc[r][a] = (add(acc[r][a][0], vr, flip * gr), add(acc[r][a][1], vi, flip * gi))


def rows_of(k):
    return slice(8 * k, 8 * k + 8)


def get_spinor(ref, index):
    return [[(ref[3 * s + a, index, :], ref[12 + 3 * s + a, index, :]) for a in range(3)] for s in range(4)]


def get_link(ref, d, index):
    return [[(ref[18 * d + 3 * a + b, index, :], ref[18 * d + 9 + 3 * a + b, index, :]) for b in range(3)] for a in range(3)]


def get_half(ref, index):
    return [[(ref[3 * s + a, index, :], ref[6 + 3 * s + a, index, :]) for a in range(3)] for s in range(2)]


def put_half(ref, index, h):
    for s in range(2):
        for a in range(3):
            ref[3 * s + a, index, :] = h[s][a][0]
            ref[6 + 3 * s + a, index, :] = h[s][a][1]


def put_spinor(ref, index, psi):
    for s in range(4):
        for a in range(3):
            ref[3 * s + a, index, :] = psi[s][a][0]
            ref[12 + 3 * s + a, index, :] = psi[s][a][1]


def iotas():
    lane = lax.broadcasted_iota(jnp.int32, (8, LANES), 1)
    row = lax.broadcasted_iota(jnp.int32, (8, LANES), 0)
    return lane, row


def shift_x(v, step):
    lane = lax.broadcasted_iota(jnp.int32, (8, LANES), 1) % 64
    if step > 0:
        return jnp.where(lane == 63, pltpu.roll(v, 63, 1), pltpu.roll(v, LANES - 1, 1))
    return jnp.where(lane == 0, pltpu.roll(v, 65, 1), pltpu.roll(v, 1, 1))


def shift_y(here, other, step):
    lane, row = iotas()
    low = row < 4
    mixed = jnp.where(low, other, here) if step > 0 else jnp.where(low, here, other)
    keep = lane >= 64 if step > 0 else lane < 64
    return pltpu.roll(jnp.where(keep, here, pltpu.roll(mixed, 4, 0)), 64, 1)


def shift_rows(v, count, step):
    return pltpu.roll(v, 8 - count if step > 0 else count, 0)


def is_even(axis):
    return lax.axis_index(axis) % 2 == 0


def outgoing(axis, up, dn):
    even = is_even(axis)
    return jnp.where(even, up, dn), jnp.where(even, dn, up)


def sent_up(axis, first, second, index):
    return jnp.where(is_even(axis), first[index], second[index])


def from_below(axis, first, second, index):
    return jnp.where(is_even(axis), second[index], first[index])


def from_above(axis, first, second, index):
    return jnp.where(is_even(axis), first[index], second[index])


def plane_copies(src, dst, sems, out=False):
    copies = []
    tiles = dst.shape[-3] // 2
    lead = (slice(None),) * (len(dst.shape) - 3)
    for t in range(2):
        for j in range(tiles):
            wide = src.at[lead + (t, slice(None), pl.ds(LANES * j, LANES))]
            packed = dst.at[lead + (2 * j + t,)]
            pair = (packed, wide) if out else (wide, packed)
            copies.append(pltpu.make_async_copy(*pair, sems.at[2 * j + t]))
    return copies


def flat(ref):
    shape = ref.shape
    lead = 1
    for n in shape[:-3]:
        lead *= n
    return ref.reshape(lead, 2 * shape[-3], LANES)


def put_face(ref, part, h):
    for s in range(2):
        for a in range(3):
            ref[pl.ds(12 * (3 * s + a) + 6 * part, 6), :] = h[s][a][0]
            ref[pl.ds(12 * (6 + 3 * s + a) + 6 * part, 6), :] = h[s][a][1]


def get_face(ref, part):
    return [[(ref[halo_row(3 * s + a, part)], ref[halo_row(6 + 3 * s + a, part)]) for a in range(3)] for s in range(2)]


def face_rows(t, z):
    return pl.ds(2 * t + z, 6, stride=4)


def halo_row(c, part):
    return (pl.ds(12 * c + 6 * part, 6), slice(None))


def faces_kernel(spinor, links, s_out, l_out, t_a, t_b, z_a, z_b, sem_s, sem_l):
    s_copies = plane_copies(spinor, s_out, sem_s)
    l_copies = plane_copies(links.at[pl.ds(2, 2)], l_out, sem_l)
    for c in s_copies + l_copies:
        c.start()
    place = lax.axis_index("ta")
    up_sign = jnp.where(place == lax.axis_size("ta") - 1, -1.0, 1.0).astype(F32)
    dn_sign = jnp.where(place == 0, -1.0, 1.0).astype(F32)
    for c in s_copies:
        c.wait()
    s_ref, l_ref = flat(s_out), flat(l_out)
    faces = []
    for part in range(2):
        faces.append(("gz", 2, z_a, z_b, part, face_rows(part, 0), face_rows(part, 1)))
        faces.append(("ta", 3, t_a, t_b, part, face_rows(0, part), face_rows(1, part)))
    for axis, mu, first, second, part, low, high in faces:
        dn = half(get_spinor(s_ref, low), mu, -1)
        if axis == "ta":
            dn = hmap(lambda v: v * dn_sign, dn)
        put_face(second, part, dn)
        put_face(first, part, half(get_spinor(s_ref, high), mu, 1))
    for c in l_copies:
        c.wait()
    for axis, mu, first, second, part, low, high in faces:
        up = cmul_dag(get_link(l_ref, mu - 2, high), get_face(first, part))
        if axis == "ta":
            up = hmap(lambda v: v * up_sign, up)
        dn = get_face(second, part)
        put_face(first, part, hmap2(lambda x, y: outgoing(axis, x, y)[0], up, dn))
        put_face(second, part, hmap2(lambda x, y: outgoing(axis, x, y)[1], up, dn))


def local_kernel(s_in, l_in, links, clover, p_out, l_out, c_ref, chi, sem_l, sem_c):
    copies_l = plane_copies(links.at[pl.ds(0, 2)], l_out, sem_l)
    copies_c = plane_copies(clover, c_ref, sem_c)
    for c in copies_l + copies_c:
        c.start()
    s_ref, l23, l01, cl = flat(s_in), flat(l_in), flat(l_out), flat(c_ref)
    _, row = iotas()
    low_z = row % 2 == 0
    low_t = (row // 2) % 2 == 0
    sign_z = jnp.where(low_z, -1.0, 1.0)
    sign_t = jnp.where(low_t, -1.0, 1.0)
    zero = jnp.zeros((8, LANES), F32)
    for k in range(3):
        psi = get_spinor(s_ref, rows_of(k))
        acc = [[(zero, zero) for _ in range(3)] for _ in range(4)]
        for mu, d, n, low, sign in ((2, 0, 1, low_z, sign_z), (3, 1, 2, low_t, sign_t)):
            u = get_link(l23, d, rows_of(k))
            ahead = cmul(u, hmap(lambda v: shift_rows(v, n, 1), half(psi, mu, -1)))
            behind = hmap(lambda v: shift_rows(v, n, -1), cmul_dag(u, half(psi, mu, 1)))
            accumulate(acc, mu, hmap2(lambda x, y: jnp.where(low, x, y), ahead, behind), sign)
        put_spinor(p_out, rows_of(k), acc)
    for c in copies_l:
        c.wait()
    for k in range(3):
        put_half(chi, rows_of(k), cmul_dag(get_link(l01, 1, rows_of(k)), half(get_spinor(s_ref, rows_of(k)), 1, 1)))
    for k in range(3):
        psi = get_spinor(s_ref, rows_of(k))
        acc = get_spinor(p_out, rows_of(k))
        u = get_link(l01, 0, rows_of(k))
        accumulate(acc, 0, cmul(u, hmap(lambda v: shift_x(v, 1), half(psi, 0, -1))), -1)
        accumulate(acc, 0, hmap(lambda v: shift_x(v, -1), cmul_dag(u, half(psi, 0, 1))), 1)
        u = get_link(l01, 1, rows_of(k))
        nxt = half(get_spinor(s_ref, rows_of((k + 1) % 3)), 1, -1)
        ahead = hmap2(lambda x, y: shift_y(x, y, 1), half(psi, 1, -1), nxt)
        accumulate(acc, 1, cmul(u, ahead), -1)
        behind = hmap2(lambda x, y: shift_y(x, y, -1), get_half(chi, rows_of(k)), get_half(chi, rows_of((k + 2) % 3)))
        accumulate(acc, 1, behind, 1)
        put_spinor(p_out, rows_of(k), acc)
    for c in copies_c:
        c.wait()
    for k in range(3):
        for chirality in range(2):
            field = [[(s_ref[6 * chirality + i, rows_of(k), :], s_ref[12 + 6 * chirality + i, rows_of(k), :])] for i in range(6)]
            for i in range(6):
                re = DIAG * field[i][0][0] - 0.5 * p_out[6 * chirality + i, rows_of(k), :]
                im = DIAG * field[i][0][1] - 0.5 * p_out[12 + 6 * chirality + i, rows_of(k), :]
                for j in range(6):
                    cr = cl[36 * chirality + 6 * i + j, rows_of(k), :]
                    ci = cl[72 + 36 * chirality + 6 * i + j, rows_of(k), :]
                    fr, fi = field[j][0]
                    re = re + (cr * fr - ci * fi)
                    im = im + (cr * fi + ci * fr)
                p_out[6 * chirality + i, rows_of(k), :] = re
                p_out[12 + 6 * chirality + i, rows_of(k), :] = im


def low_rows(mu):
    row = lax.broadcasted_iota(jnp.int32, (8, LANES), 0)
    return (row if mu == 2 else row // 2) % 2 == 0


def spread(dst, mu, level, value):
    for c in range(12):
        for part in range(2):
            first = 2 * part + level if mu == 2 else 2 * level + part
            dst[c, pl.ds(first, 6, stride=4), :] = value(c, part)


def add_halo(acc, mu, u, h):
    low = low_rows(mu)
    term = hmap2(lambda x, y: -0.5 * jnp.where(low, x, y), h, cmul(u, h))
    accumulate(acc, mu, term, jnp.where(low, 1.0, -1.0))


def halo_kernel(mu, p_in, l_in, first, second, a_out, face, halo):
    axis = "gz" if mu == 2 else "ta"
    l23 = flat(l_in)
    a_ref = flat(a_out) if len(a_out.shape) > 3 else a_out
    spread(halo, mu, 0, lambda c, part: from_below(axis, first, second, halo_row(c, part)))
    spread(halo, mu, 1, lambda c, part: from_above(axis, first, second, halo_row(c, part)))
    for k in range(3):
        acc = get_spinor(p_in, rows_of(k))
        add_halo(acc, mu, get_link(l23, mu - 2, rows_of(k)), get_half(halo, rows_of(k)))
        put_spinor(a_ref, rows_of(k), acc)
    dn_sign = jnp.where(lax.axis_index("ta") == 0, -1.0, 1.0).astype(F32)
    for part in range(2):
        if mu == 3:
            put_face(face, part, half(get_spinor(a_ref, face_rows(part, 0)), 2, 1))
        else:
            out = half(get_spinor(a_ref, face_rows(0, part)), 3, 1)
            put_face(face, part, hmap(lambda v: v * dn_sign, out))


def mid_kernel(*refs):
    halo_kernel(3, *refs)


def finish_kernel(*refs):
    halo_kernel(2, *refs)


def outer(left, right, total=None):
    out = []
    for a in range(3):
        row = []
        for b in range(3):
            re, im = (None, None) if total is None else total[a][b]
            for s in range(2):
                lr, li = left[s][a]
                rr, ri = right[s][b]
                r = lr * rr + li * ri
                i = li * rr - lr * ri
                re = r if re is None else re + r
                im = i if im is None else im + i
            row.append((re, im))
        out.append(row)
    return out


def put_force(ref, d, index, u, m):
    w = []
    for a in range(3):
        row = []
        for b in range(3):
            re = im = None
            for c in range(3):
                ur, ui = u[a][c]
                mr, mi = m[c][b]
                i = ur * mi + ui * mr
                im = i if im is None else im + i
                if a != b:
                    r = ur * mr - ui * mi
                    re = r if re is None else re + r
            row.append((re, im))
        w.append(row)
    third = (w[0][0][1] + w[1][1][1] + w[2][2][1]) * (1.0 / 3.0)
    for a in range(3):
        ref[18 * d + 4 * a, index, :] = jnp.zeros((8, LANES), F32)
        ref[18 * d + 9 + 4 * a, index, :] = w[a][a][1] - third
        for b in range(a + 1, 3):
            re = 0.5 * (w[a][b][0] - w[b][a][0])
            im = 0.5 * (w[a][b][1] + w[b][a][1])
            ref[18 * d + 3 * a + b, index, :] = re
            ref[18 * d + 3 * b + a, index, :] = -re
            ref[18 * d + 9 + 3 * a + b, index, :] = im
            ref[18 * d + 9 + 3 * b + a, index, :] = im


def get_matrix(ref, d, index):
    return get_link(ref, d, index)


def put_matrix(ref, d, index, m):
    for a in range(3):
        for b in range(3):
            ref[18 * d + 3 * a + b, index, :] = m[a][b][0]
            ref[18 * d + 9 + 3 * a + b, index, :] = m[a][b][1]


def plane_kernel(s_in, a_in, l_in, t_a, t_b, z_a, z_b, applied, force, m_out, f_ref, halo, sem_a, sem_f):
    copies = plane_copies(applied, a_in, sem_a, out=True)
    for c in copies:
        c.start()
    s_ref, a_ref, l01, f = flat(s_in), flat(a_in), flat(l_in), flat(f_ref)
    for k in range(3):
        psi = get_spinor(s_ref, rows_of(k))
        app = get_spinor(a_ref, rows_of(k))
        m = outer(hmap(lambda v: shift_x(v, 1), half(psi, 0, -1)), half(app, 0, -1))
        m = outer(hmap(lambda v: shift_x(v, 1), half(app, 0, 1)), half(psi, 0, 1), m)
        put_force(f, 0, rows_of(k), get_link(l01, 0, rows_of(k)), m)
        psi_n = half(get_spinor(s_ref, rows_of((k + 1) % 3)), 1, -1)
        app_n = half(get_spinor(a_ref, rows_of((k + 1) % 3)), 1, 1)
        m = outer(hmap2(lambda x, y: shift_y(x, y, 1), half(psi, 1, -1), psi_n), half(app, 1, -1))
        m = outer(hmap2(lambda x, y: shift_y(x, y, 1), half(app, 1, 1), app_n), half(psi, 1, 1), m)
        put_force(f, 1, rows_of(k), get_link(l01, 1, rows_of(k)), m)
    out = plane_copies(force.at[pl.ds(0, 2)], f_ref, sem_f, out=True)
    for c in out:
        c.start()
    for mu, axis, first, second in ((2, "gz", z_a, z_b), (3, "ta", t_a, t_b)):
        low = low_rows(mu)
        spread(halo, mu, 1, lambda c, part: from_above(axis, first, second, halo_row(c, part)))
        for k in range(3):
            psi = get_spinor(s_ref, rows_of(k))
            app = get_spinor(a_ref, rows_of(k))
            near = hmap(lambda v: shift_rows(v, mu - 1, 1), half(psi, mu, -1))
            ahead = hmap2(lambda x, y: jnp.where(low, x, y), near, get_half(halo, rows_of(k)))
            m = outer(ahead, half(app, mu, -1))
            ahead = hmap(lambda v: jnp.where(low, shift_rows(v, mu - 1, 1), 0.0), half(app, mu, 1))
            m = outer(ahead, half(psi, mu, 1), m)
            put_matrix(m_out, mu - 2, rows_of(k), m)
    for c in copies + out:
        c.wait()


def edge_kernel(s_in, l_in, m_in, a_t, a_z, z_a, z_b, force_in, force, f_ref, halo, sem_f):
    s_ref, l23, f = flat(s_in), flat(l_in), flat(f_ref)
    out = []
    for d, mu in ((1, 3), (0, 2)):
        low = low_rows(mu)
        if mu == 3:
            spread(halo, mu, 1, lambda c, part: a_t[halo_row(c, part)])
        else:
            spread(halo, mu, 1, lambda c, part: a_z[halo_row(c, part)] - sent_up("gz", z_a, z_b, halo_row(c, part)))
        for k in range(3):
            psi = half(get_spinor(s_ref, rows_of(k)), mu, 1)
            ahead = hmap(lambda v: jnp.where(low, 0.0, v), get_half(halo, rows_of(k)))
            m = outer(ahead, psi, get_matrix(m_in, d, rows_of(k)))
            put_force(f, d, rows_of(k), get_link(l23, d, rows_of(k)), m)
        copies = plane_copies(force.at[pl.ds(mu, 1)], f_ref.at[pl.ds(d, 1)], sem_f.at[d], out=True)
        for c in copies:
            c.start()
        out += copies
    for c in out:
        c.wait()


HBM = pl.BlockSpec(memory_space=pltpu.HBM)
VMEM = pl.BlockSpec(memory_space=pltpu.VMEM)
LIMIT = 12 * 1024 * 1024


def call(kernel, ins, outs, scratch, args, aliases=None):
    return pl.pallas_call(
        kernel,
        out_shape=tuple(jax.ShapeDtypeStruct(shape, F32) for shape, _ in outs),
        in_specs=list(ins),
        out_specs=tuple(spec for _, spec in outs),
        scratch_shapes=list(scratch),
        compiler_params=pltpu.CompilerParams(vmem_limit_bytes=LIMIT),
        input_output_aliases=aliases or {},
    )(*args)


def moved(value, axis, step):
    count = lax.axis_size(axis)
    return lax.ppermute(value, axis, [(i, (i + step) % count) for i in range(count)])


def swapped(value, axis, start):
    count = lax.axis_size(axis)
    pairs = [(i % count, (i + 1) % count) for i in range(start, count + start, 2)]
    return lax.ppermute(value, axis, pairs + [(b, a) for a, b in pairs])


def steps(spinor, links, clover):
    tiles = spinor.shape[-1] // LANES
    packed = (2 * tiles, 2, LANES)
    s_shape = (2, 4, 3) + packed
    l_shape = (2, 2, 3, 3) + packed
    c_shape = (2, 2, 6, 6) + packed
    rows = (4 * tiles, LANES)
    face = ((24 * tiles, LANES), VMEM)
    halo = pltpu.VMEM((12,) + rows, F32)
    dma = pltpu.SemaphoreType.DMA((2 * tiles,))
    spinor, links, clover = (pltpu.with_memory_space_constraint(x, pltpu.HBM) for x in (spinor, links, clover))
    s, l23, t_a, t_b, z_a, z_b = call(
        faces_kernel, (HBM, HBM), ((s_shape, VMEM), (l_shape, VMEM), face, face, face, face),
        (dma, dma), (spinor, links),
    )
    z_sent = (z_a, z_b)
    z_a = swapped(z_a, "gz", 0)
    z_b = swapped(z_b, "gz", 1)
    t_a = swapped(t_a, "ta", 0)
    t_b = swapped(t_b, "ta", 1)
    p, l01 = call(
        local_kernel, (VMEM, VMEM, HBM, HBM), (((24,) + rows, VMEM), (l_shape, VMEM)),
        (pltpu.VMEM(c_shape, F32), halo, dma, dma), (s, l23, links, clover),
    )
    p, a_z = call(mid_kernel, (VMEM,) * 4, (((24,) + rows, VMEM), face), (halo,), (p, l23, t_a, t_b))
    a_z = moved(a_z, "gz", -1)
    a, a_t = call(finish_kernel, (VMEM,) * 4, ((s_shape, VMEM), face), (halo,), (p, l23, z_a, z_b))
    a_t = moved(a_t, "ta", -1)
    applied, force, m = call(
        plane_kernel, (VMEM,) * 7, ((spinor.shape, HBM), (links.shape, HBM), ((36,) + rows, VMEM)),
        (pltpu.VMEM(l_shape, F32), halo, dma, dma), (s, a, l01, t_a, t_b, z_a, z_b),
    )
    (force,) = call(
        edge_kernel, (VMEM,) * 7 + (HBM,), ((links.shape, HBM),),
        (pltpu.VMEM(l_shape, F32), halo, pltpu.SemaphoreType.DMA((2, 2 * tiles))),
        (s, l23, m, a_t, a_z) + z_sent + (force,), {7: 0},
    )
    return applied, force


def solution(mesh):
    spin = P(None, None, None, "ta", "gz", None)
    link = P(None, None, None, None, "ta", "gz", None)
    return jax.shard_map(steps, mesh=mesh, in_specs=(spin, link, link), out_specs=(spin, link), check_vma=False)
```
